512 devices in a mesh: section: 32 (over x, y_hi, core), dp: 16 (over y_lo, z).
Axes of the slice: x: 4, y: 8 (y_hi: 4, y_lo: 2; y = y_hi * 2 + y_lo), z: 8, core: 2. Of those that a mesh axis runs over, the one named last changes fastest.
Arguments:
- out_pair: float32 [2048, 2048], P('dp'), may hold values from -6 to 6
- out_grad: bfloat16 [2048, 2048], P('dp'), may hold values from -6 to 6
- f_weight: bfloat16 [32, 1024, 1024], P('section', 'dp'), may hold values from -0.09375 to 0.09375
- g_weight: bfloat16 [32, 1024, 1024], P('section', 'dp'), may hold values from -0.09375 to 0.09375
- gains: float32 [32, 2, 1024], P('section'), may hold values from 0.1 to 1.9
Outputs:
- in_pair: float32 [32, 2048, 2048], P('section', 'dp')
- in_grad: bfloat16 [32, 2048, 2048], P('section', 'dp')
- f_grad: float32 [32, 1024, 1024], P('section', 'dp')
- g_grad: float32 [32, 1024, 1024], P('section', 'dp')
- gains_grad: float32 [32, 2, 1024], P('section')
The draws below stay inside these ranges and needn't reach their ends.
All inputs are finite; a program needn't handle non-finite values.
Results may differ from the reference program's by a relative error of at most 0.04.
Values may be sent and summed in bfloat16 or wider, within the bound.
A program may use at most 64 MiB of HBM per device.

```python
import jax
import jax.numpy as jnp
from jax import lax

DH = 1024
TOK_DEV = 128
SECTIONS = 32
TOKENS = 2048
N_SECTION = 32
N_DP = 16


def steps_of(key, extent, shards, smallest, top_value):
    gain, own = 1.0, jax.random.fold_in(key, 6)
    for dim, parts in shards:
        steps = jnp.exp(jax.random.uniform(jax.random.fold_in(own, dim), (parts,), jnp.float32, smallest / len(shards), top_value / len(shards)))
        gain = gain * jnp.repeat(steps, extent[dim] // parts).reshape([-1 if axis == dim else 1 for axis in range(len(extent))])
    return gain


def centred(key, dims, width, reach, shards=(), kind=jnp.bfloat16):
    result = width * jax.random.normal(key, dims, jnp.float32)
    if shards:
        result = result * steps_of(key, dims, shards, -0.22, 0.18)
    return jnp.clip(result, -reach, reach).astype(kind)


def setup_inputs(seed: int = 0) -> dict:
    seeds = jax.random.split(jax.random.key(seed), 6)
    out_pair = centred(seeds[0], (TOKENS, 2 * DH), 1.0, 6.0, ((0, 16),), jnp.float32)
    out_grad = centred(seeds[1], (TOKENS, 2 * DH), 1.0, 6.0, ((0, 16),))
    f_weight = centred(seeds[2], (SECTIONS, DH, DH), (4 * DH) ** -0.5, 0.09375, ((0, 32), (1, 16)))
    g_weight = centred(seeds[3], (SECTIONS, DH, DH), (4 * DH) ** -0.5, 0.09375, ((0, 32), (1, 16)))
    gains = jnp.clip(1.0 + 0.18 * jax.random.normal(seeds[4], (SECTIONS, 2, DH), jnp.float32), 0.1, 1.9)
    return {"out_pair": out_pair, "out_grad": out_grad, "f_weight": f_weight, "g_weight": g_weight, "gains": gains}


offset = 0.25

def silu_parts(pre_values):
    sigmoid_value = jax.nn.sigmoid(pre_values)
    return (pre_values * sigmoid_value, sigmoid_value * (1.0 + pre_values * (1.0 - sigmoid_value)))

def normalize(values, gain_row):
    inv_scale = lax.rsqrt(lax.optimization_barrier(jnp.mean(values * values, axis=-1, keepdims=True)) + offset)
    return ((values * inv_scale * gain_row).astype(jnp.bfloat16), inv_scale)

def norm_back(values, inv_scale, gain_row, upstream):
    weighted = gain_row * upstream
    cubed = inv_scale * inv_scale * inv_scale
    return inv_scale * weighted - values * cubed * lax.optimization_barrier(jnp.mean(weighted * values, axis=-1, keepdims=True))

def coupling_back(upper_out, lower_out, upper_grad, lower_grad, w_first, w_second, gain_pair):
    normed_second, scale_second = normalize(upper_out, gain_pair[1])
    pre_second = jnp.dot(normed_second, w_second, preferred_element_type=jnp.float32)
    act_second, slope_second = silu_parts(pre_second)
    lower_in = lower_out - act_second
    normed_first, scale_first = normalize(lower_in, gain_pair[0])
    pre_first = jnp.dot(normed_first, w_first, preferred_element_type=jnp.float32)
    act_first, slope_first = silu_parts(pre_first)
    upper_in = upper_out - act_first
    delta_second = (lower_grad * slope_second).astype(jnp.bfloat16)
    back_second = jnp.dot(delta_second, w_second.T, preferred_element_type=jnp.float32)
    through = upper_grad + norm_back(upper_out, scale_second, gain_pair[1], back_second)
    delta_first = (through * slope_first).astype(jnp.bfloat16)
    back_first = jnp.dot(delta_first, w_first.T, preferred_element_type=jnp.float32)
    lower_total = lower_grad + norm_back(lower_in, scale_first, gain_pair[0], back_first)
    gain_terms = jnp.stack([lax.optimization_barrier(jnp.sum(back_first * lower_in * scale_first, axis=0)), lax.optimization_barrier(jnp.sum(back_second * upper_out * scale_second, axis=0))])
    return (upper_in, lower_in, through.astype(jnp.bfloat16), lower_total.astype(jnp.bfloat16), normed_first, delta_first, normed_second, delta_second, gain_terms)

def replica_sum(normed, delta):
    left_side = normed.reshape(N_DP, TOK_DEV, -1).astype(jnp.float32)
    right_side = delta.reshape(N_DP, TOK_DEV, -1).astype(jnp.float32)
    partial_sums = jnp.einsum('rtd,rte->rde', left_side, right_side)
    rounded = lax.optimization_barrier(partial_sums.astype(jnp.bfloat16))
    return lax.optimization_barrier(jnp.sum(rounded.astype(jnp.float32), axis=0))

def reference(out_pair, out_grad, f_weight, g_weight, gains):
    channels = out_pair.shape[1] // 2
    pair_now = out_pair
    grad_now = out_grad
    pairs, grads, first_sums, second_sums, gain_sums = ([], [], [], [], [])
    for layer_index in range(N_SECTION - 1, -1, -1):
        results = coupling_back(pair_now[:, :channels], pair_now[:, channels:], grad_now[:, :channels].astype(jnp.float32), grad_now[:, channels:].astype(jnp.float32), f_weight[layer_index], g_weight[layer_index], gains[layer_index])
        pair_now = jnp.concatenate([results[0], results[1]], axis=1)
        grad_now = jnp.concatenate([results[2], results[3]], axis=1)
        pairs.append(pair_now)
        grads.append(grad_now)
        first_sums.append(replica_sum(results[4], results[5]))
        second_sums.append(replica_sum(results[6], results[7]))
        gain_sums.append(results[8])
    return (jnp.stack(pairs[::-1]), jnp.stack(grads[::-1]), jnp.stack(first_sums[::-1]), jnp.stack(second_sums[::-1]), jnp.stack(gain_sums[::-1]))
```

```python
import functools

import jax
import jax.numpy as jnp
from jax import lax
from jax.experimental import pallas as pl
from jax.experimental.pallas import tpu as pltpu
from jax.sharding import PartitionSpec as P

offset = 0.25
MESH = pl.DeviceIdType.MESH
f32, bf16 = jnp.float32, jnp.bfloat16


def kernel(
    n, sections, blocks,
    pair_ref, grad_ref, fw_ref, gw_ref, gains_ref,
    in_pair_ref, in_grad_ref, f_out, g_out, gain_out,
    wf, wg, wft, wgt, rx, tx, y1s, pres, slopes, norm_full, norm_cat, delta_cat, sums, rs_rx, rs_tx, gain_parts,
    own_sem, zs, zr, os_, or_, ys, yr, y2s, y2r, p_send, p_recv, n_send, n_recv, d_send, d_recv, r_send, r_recv, c_send, c_recv,
):
    s, d = lax.axis_index("section"), lax.axis_index("dp")
    is_last = s == sections - 1
    has_below = s > 0
    not_last = jnp.logical_not(is_last)
    tokens = pair_ref.shape[0]
    h = pair_ref.shape[1] // 2
    part = fw_ref.shape[0]
    rows_per = tokens // blocks
    zn = n // 2
    hh = zn * part
    z, row = lax.rem(d, zn), d // zn
    beside = (1 - row) * zn + z
    ring_next = (row * zn + lax.rem(z + 1, zn), row * zn + lax.rem(z + zn - 1, zn))

    barrier = pltpu.get_barrier_semaphore()
    for k in range(1, n):
        pl.semaphore_signal(barrier, inc=1, device_id=(s, lax.rem(d + k, n)), device_id_type=MESH)

    @pl.when(has_below)
    def _():
        pl.semaphore_signal(barrier, inc=1, device_id=(s - 1, d), device_id_type=MESH)

    @pl.when(not_last)
    def _():
        pl.semaphore_signal(barrier, inc=1, device_id=(s + 1, d), device_id_type=MESH)

    pl.semaphore_wait(barrier, n - 1 + has_below.astype(jnp.int32) + not_last.astype(jnp.int32))

    def remote(src, dst, send, recv, target):
        return pltpu.make_async_remote_copy(
            src_ref=src, dst_ref=dst, send_sem=send, recv_sem=recv,
            device_id=target, device_id_type=MESH,
        )

    def wait_bytes(ref, sem):
        pltpu.make_async_copy(ref, ref, sem).wait()

    fulls, owns, turned = (wg, wf), (gw_ref, fw_ref), (wgt, wft)
    c1 = h * 5 // 8
    cols_1, cols_2, all_cols = pl.ds(0, c1), pl.ds(c1, h - c1), pl.ds(0, h)
    reach = ((zn // 2, zn - 1 - zn // 2), (zn - 1 - zn // 2, zn // 2))

    def ring_pos(way, k):
        return lax.rem(z + (zn - k if way == 0 else k), zn)

    def shard(a, line, pos, cols):
        return fulls[a].at[pl.ds(pl.multiple_of((line * zn + pos) * part, part), part), cols]

    def own_hop(a, way, k):
        dst = shard(a, row, ring_pos(way, k), all_cols)
        return remote(owns[a] if k == 0 else dst, dst, zs.at[a, way, k], zr.at[a, way, k], (s, ring_next[way]))

    def other_hop(a, way, k):
        ref = shard(a, 1 - row, ring_pos(way, k), cols_2)
        return remote(ref, ref, os_.at[a, way, k], or_.at[a, way, k], (s, ring_next[way]))

    def cross(a, way, k):
        dst = shard(a, row, ring_pos(way, k), cols_1)
        return remote(owns[a].at[:, cols_1] if k == 0 else dst, dst, ys.at[a, way, k], yr.at[a, way, k], (s, beside))

    def cross_2(a):
        return remote(owns[a].at[:, cols_2], shard(a, row, z, cols_2), y2s.at[a], y2r.at[a], (s, beside))

    own_copies = [pltpu.make_async_copy(owns[a], shard(a, row, z, all_cols), own_sem.at[a]) for a in range(2)]
    for a in range(2):
        cross_2(a).start()
        for way in range(2):
            own_hop(a, way, 0).start()
        cross(a, 0, 0).start()
        own_copies[a].start()

    parity = lax.rem(z, 2)
    pairs = zn // 2

    def turn(a, line, step):
        shift = (0, 2 * parity - 1, 1 - 2 * parity, 2)[step]
        chunk = line * pairs + lax.rem(z // 2 + shift + pairs, pairs)
        span = pl.ds(pl.multiple_of(chunk * 2 * part, 2 * part), 2 * part)
        turned[a][:, span] = fulls[a][span, :].T

    def take_cross(a, k):
        for way in range(2):
            if (k > 0 or way == 0) and k <= reach[a][way]:
                wait_bytes(shard(a, 1 - row, ring_pos(way, k), cols_1), yr.at[a, way, k])

    for a in range(2):
        wait_bytes(shard(a, 1 - row, z, cols_2), y2r.at[a])
        for way in range(2):
            other_hop(a, way, 0).start()
    for a in range(2):
        own_copies[a].wait()

    for k in range(1, pairs + 1):
        for a in range(2):
            for way in range(2):
                if k <= reach[a][way]:
                    wait_bytes(shard(a, row, ring_pos(way, k), all_cols), zr.at[a, way, k - 1])
                    if k < reach[a][way]:
                        own_hop(a, way, k).start()
                    cross(a, way, k).start()
            for way in range(2):
                if k <= reach[a][way]:
                    wait_bytes(shard(a, 1 - row, ring_pos(way, k), cols_2), or_.at[a, way, k - 1])
                    if k < reach[a][way]:
                        other_hop(a, way, k).start()
        for a in range(2):
            take_cross(a, k - 1)
            turn(a, row, k - 1)
            if k > 1:
                turn(a, 1 - row, k - 2)
    for a in range(2):
        take_cross(a, pairs)
        turn(a, 1 - row, pairs - 1)

    gain_out[...] = jnp.zeros_like(gain_out)

    def incoming(i, b):
        return pl.ds(pl.multiple_of(b * rows_per, rows_per), rows_per)

    def await_from_above(i, b):
        @pl.when(not_last)
        def _():
            wait_bytes(rx.at[i, incoming(i, b)], p_recv.at[i, b])

    def give(i, b, rows, values):
        tx[i, rows] = values.astype(bf16)

        @pl.when(has_below)
        def _():
            remote(tx.at[i, rows], rx.at[i, rows], p_send.at[i], p_recv.at[i, b], (s - 1, d)).start()

    def share_norm(a, b, rows, normed):
        norm_full[a, rows] = normed
        remote(
            norm_full.at[a, rows, pl.ds(pl.multiple_of((1 - row) * hh, hh), hh)], norm_cat.at[a, 1, rows],
            n_send.at[a], n_recv.at[a], (s, beside),
        ).start()

    def share_delta(a, b, rows):
        remote(
            delta_cat.at[a, 0, rows], delta_cat.at[a, 1, rows],
            d_send.at[a], d_recv.at[a], (s, beside),
        ).start()

    first, second = pl.ds(0, h), pl.ds(h, h)

    def scale_of(values):
        return lax.rsqrt(jnp.sum(values * values, axis=-1, keepdims=True) * (1.0 / h) + offset)

    def block(b, carry):
        rows = pl.ds(pl.multiple_of(b * rows_per, rows_per), rows_per)
        gain_f, gain_g = gains_ref[0:1, :], gains_ref[1:2, :]
        await_from_above(1, b)
        await_from_above(0, b)
        y1 = jnp.where(is_last, pair_ref[rows, first], rx[0, rows].astype(f32))
        y2 = jnp.where(is_last, pair_ref[rows, second], rx[1, rows].astype(f32))
        y1s[...] = y1
        r1 = scale_of(y1)
        pre_g = jnp.dot((y1 * gain_g).astype(bf16), wg[...], preferred_element_type=f32) * r1
        sig_g = jax.nn.sigmoid(pre_g)
        x2 = y2 - pre_g * sig_g
        give(1, b, rows, x2)
        r2 = scale_of(x2)
        pre_f = jnp.dot((x2 * gain_f).astype(bf16), wf[...], preferred_element_type=f32) * r2
        sig_f = jax.nn.sigmoid(pre_f)
        x1 = y1 - pre_f * sig_f
        give(0, b, rows, x1)
        in_pair_ref[rows, first] = x1
        in_pair_ref[rows, second] = x2
        pres[0] = pre_g
        pres[1] = pre_f
        slopes[0] = sig_g * (1.0 + pre_g * (1.0 - sig_g))
        slopes[1] = sig_f * (1.0 + pre_f * (1.0 - sig_f))
        share_norm(0, b, rows, (y1 * r1 * gain_g).astype(bf16))
        share_norm(1, b, rows, (x2 * r2 * gain_f).astype(bf16))

        await_from_above(2, b)
        await_from_above(3, b)
        gy1 = jnp.where(is_last, grad_ref[rows, first].astype(f32), rx[2, rows].astype(f32))
        gy2 = jnp.where(is_last, grad_ref[rows, second].astype(f32), rx[3, rows].astype(f32))
        delta_g = (gy2 * slopes[0]).astype(bf16)
        back_g = jnp.dot(delta_g, wgt[...], preferred_element_type=f32)
        mean_g = jnp.sum(delta_g.astype(f32) * pres[0], axis=-1, keepdims=True) * (1.0 / h)
        y1 = y1s[...]
        gz = gy1 + (r1 * gain_g) * back_g - y1 * (mean_g * (r1 * r1))
        give(2, b, rows, gz)
        delta_f = (gz * slopes[1]).astype(bf16)
        back_f = jnp.dot(delta_f, wft[...], preferred_element_type=f32)
        mean_f = jnp.sum(delta_f.astype(f32) * pres[1], axis=-1, keepdims=True) * (1.0 / h)
        x2 = in_pair_ref[rows, second]
        gx2 = gy2 + (r2 * gain_f) * back_f - x2 * (mean_f * (r2 * r2))
        give(3, b, rows, gx2)
        in_grad_ref[rows, first] = gz.astype(bf16)
        in_grad_ref[rows, second] = gx2.astype(bf16)
        delta_cat[0, 0, rows] = delta_g
        delta_cat[1, 0, rows] = delta_f
        share_delta(0, b, rows)
        share_delta(1, b, rows)
        gain_out[1:2, :] += jnp.sum(back_g * (y1 * r1), axis=0, keepdims=True)
        gain_out[0:1, :] += jnp.sum(back_f * (x2 * r2), axis=0, keepdims=True)
        return carry

    lax.fori_loop(0, blocks, block, 0)

    gain_parts[d] = gain_out[...]
    for k in range(1, n):
        remote(gain_parts.at[d], gain_parts.at[d], c_send, c_recv, (s, lax.rem(d + k, n))).start()

    for a in range(2):
        norm_cat[a, 0] = norm_full[a, :, pl.ds(pl.multiple_of(row * hh, hh), hh)]

    def slot(pos):
        return pl.ds(pl.multiple_of(pos * part, part), part)

    def sum_hop(a, way, t):
        return remote(rs_tx.at[a, way, t], rs_rx.at[a, way, t], r_send.at[a, way, t], r_recv.at[a, way, t], (s, ring_next[way]))

    def sum_pos(a, way, t):
        far = reach[a][way] - t
        return lax.rem(z + (far if way == 0 else zn - far), zn)

    for a in range(2):
        wait_bytes(norm_cat.at[a, 1], n_recv.at[a])
        wait_bytes(delta_cat.at[a, 1], d_recv.at[a])
        sums[a] = lax.dot_general(
            norm_cat[a].reshape(2 * tokens, hh), delta_cat[a].reshape(2 * tokens, h),
            (((0,), (0,)), ((), ())), preferred_element_type=f32,
        )
        for way in range(2):
            if reach[a][way] > 0:
                rs_tx[a, way, 0] = sums[a, slot(sum_pos(a, way, 0))].astype(bf16)
                sum_hop(a, way, 0).start()
    for t in range(1, pairs):
        for a in range(2):
            for way in range(2):
                if t < reach[a][way]:
                    wait_bytes(rs_rx.at[a, way, t - 1], r_recv.at[a, way, t - 1])
                    rs_tx[a, way, t] = (sums[a, slot(sum_pos(a, way, t))] + rs_rx[a, way, t - 1].astype(f32)).astype(bf16)
                    sum_hop(a, way, t).start()
    for a, out in ((0, g_out), (1, f_out)):
        total = sums[a, slot(z)]
        for way in range(2):
            if reach[a][way] > 0:
                last = reach[a][way] - 1
                wait_bytes(rs_rx.at[a, way, last], r_recv.at[a, way, last])
                total = total + rs_rx[a, way, last].astype(f32)
        out[...] = total

    others = pl.ds(0, n - 1)
    wait_bytes(gain_parts.at[others], c_recv)
    total = gain_parts[0]
    for e in range(1, n):
        total = total + gain_parts[e]
    gain_out[...] = total

    wait_bytes(gain_parts.at[others], c_send)
    for a in range(2):
        wait_bytes(norm_cat.at[a, 1], n_send.at[a])
        wait_bytes(delta_cat.at[a, 1], d_send.at[a])
        cross_2(a).wait_send()
        cross(a, 0, 0).wait_send()
        for way in range(2):
            for k in range(reach[a][way]):
                own_hop(a, way, k).wait_send()
                other_hop(a, way, k).wait_send()
                cross(a, way, k + 1).wait_send()
                sum_hop(a, way, k).wait_send()

    @pl.when(has_below)
    def _():
        for i in range(4):
            wait_bytes(tx.at[i], p_send.at[i])


def shards(out_pair, out_grad, f_weight, g_weight, gains):
    n, sections = lax.axis_size("dp"), lax.axis_size("section")
    tokens, width = out_pair.shape
    h = width // 2
    part = f_weight.shape[1]
    blocks = 4
    zn = n // 2
    hops = max(zn // 2, 1)
    rows_per = tokens // blocks
    vmem = pl.BlockSpec(memory_space=pltpu.VMEM)
    dma = pltpu.SemaphoreType.DMA
    outs = pl.pallas_call(
        functools.partial(kernel, n, sections, blocks),
        out_shape=(
            jax.ShapeDtypeStruct((tokens, width), f32),
            jax.ShapeDtypeStruct((tokens, width), bf16),
            jax.ShapeDtypeStruct((part, h), f32),
            jax.ShapeDtypeStruct((part, h), f32),
            jax.ShapeDtypeStruct((2, h), f32),
        ),
        in_specs=[vmem] * 5,
        out_specs=[vmem] * 5,
        scratch_shapes=[
            pltpu.VMEM((h, h), bf16),
            pltpu.VMEM((h, h), bf16),
            pltpu.VMEM((h, h), bf16),
            pltpu.VMEM((h, h), bf16),
            pltpu.VMEM((4, tokens, h), bf16),
            pltpu.VMEM((4, tokens, h), bf16),
            pltpu.VMEM((rows_per, h), f32),
            pltpu.VMEM((2, rows_per, h), f32),
            pltpu.VMEM((2, rows_per, h), f32),
            pltpu.VMEM((2, tokens, h), bf16),
            pltpu.VMEM((2, 2, tokens, zn * part), bf16),
            pltpu.VMEM((2, 2, tokens, h), bf16),
            pltpu.VMEM((2, zn * part, h), f32),
            pltpu.VMEM((2, 2, hops, part, h), bf16),
            pltpu.VMEM((2, 2, hops, part, h), bf16),
            pltpu.VMEM((n, 2, h), f32),
            dma((2,)),
            dma((2, 2, hops)),
            dma((2, 2, hops)),
            dma((2, 2, hops)),
            dma((2, 2, hops)),
            dma((2, 2, hops + 1)),
            dma((2, 2, hops + 1)),
            dma((2,)),
            dma((2,)),
            dma((4,)),
            dma((4, blocks)),
            dma((2,)),
            dma((2,)),
            dma((2,)),
            dma((2,)),
            dma((2, 2, hops)),
            dma((2, 2, hops)),
            dma,
            dma,
        ],
        compiler_params=pltpu.CompilerParams(
            collective_id=0, has_side_effects=True, vmem_limit_bytes=60 * 1024 * 1024
        ),
    )(out_pair, out_grad, f_weight[0], g_weight[0], gains[0])
    return tuple(out[None] for out in outs)


def solution(mesh):
    placed = (
        P("dp", None),
        P("dp", None),
        P("section", "dp", None),
        P("section", "dp", None),
        P("section", None, None),
    )
    return jax.shard_map(
        shards,
        mesh=mesh,
        in_specs=placed,
        out_specs=(
            P("section", "dp", None),
            P("section", "dp", None),
            P("section", "dp", None),
            P("section", "dp", None),
            P("section", None, None),
        ),
        check_vma=False,
    )
```

```python
import functools

import jax
import jax.numpy as jnp
from jax import lax
from jax.experimental import pallas as pl
from jax.experimental.pallas import tpu as pltpu
from jax.sharding import PartitionSpec as P

offset = 0.25
MESH = pl.DeviceIdType.MESH
f32, bf16 = jnp.float32, jnp.bfloat16


def kernel(
    n, sections, blocks,
    pair_ref, grad_ref, fw_ref, gw_ref, gains_ref,
    in_pair_ref, in_grad_ref, f_out, g_out, gain_out,
    wf, wg, wft, wgt, rx, tx, y1s, pres, slopes, norm_full, norm_cat, delta_cat, sums, rs_rx, rs_tx, gain_parts,
    own_sem, zs, zr, os_, or_, ys, yr, y2s, y2r, p_send, p_recv, n_send, n_recv, d_send, d_recv, r_send, r_recv, c_send, c_recv, turn_sem,
):
    s, d = lax.axis_index("section"), lax.axis_index("dp")
    is_last = s == sections - 1
    has_below = s > 0
    not_last = jnp.logical_not(is_last)
    tokens = pair_ref.shape[0]
    h = pair_ref.shape[1] // 2
    part = fw_ref.shape[0]
    rows_per = tokens // blocks
    zn = n // 2
    hh = zn * part
    z, row = lax.rem(d, zn), d // zn
    beside = (1 - row) * zn + z
    ring_next = (row * zn + lax.rem(z + 1, zn), row * zn + lax.rem(z + zn - 1, zn))

    barrier = pltpu.get_barrier_semaphore()
    for k in range(1, n):
        pl.semaphore_signal(barrier, inc=1, device_id=(s, lax.rem(d + k, n)), device_id_type=MESH)

    @pl.when(has_below)
    def _():
        pl.semaphore_signal(barrier, inc=1, device_id=(s - 1, d), device_id_type=MESH)

    @pl.when(not_last)
    def _():
        pl.semaphore_signal(barrier, inc=1, device_id=(s + 1, d), device_id_type=MESH)

    pl.semaphore_wait(barrier, n - 1 + has_below.astype(jnp.int32) + not_last.astype(jnp.int32))

    def remote(src, dst, send, recv, target):
        return pltpu.make_async_remote_copy(
            src_ref=src, dst_ref=dst, send_sem=send, recv_sem=recv,
            device_id=target, device_id_type=MESH,
        )

    def wait_bytes(ref, sem):
        pltpu.make_async_copy(ref, ref, sem).wait()

    fulls, owns, turned = (wg, wf), (gw_ref, fw_ref), (wgt, wft)
    c1 = h * 5 // 8
    cols_1, cols_2, all_cols = pl.ds(0, c1), pl.ds(c1, h - c1), pl.ds(0, h)
    reach = ((zn // 2, zn - 1 - zn // 2), (zn - 1 - zn // 2, zn // 2))

    def ring_pos(way, k):
        return lax.rem(z + (zn - k if way == 0 else k), zn)

    def shard(a, line, pos, cols):
        return fulls[a].at[pl.ds(pl.multiple_of((line * zn + pos) * part, part), part), cols]

    def own_hop(a, way, k):
        dst = shard(a, row, ring_pos(way, k), all_cols)
        return remote(owns[a] if k == 0 else dst, dst, zs.at[a, way, k], zr.at[a, way, k], (s, ring_next[way]))

    def other_hop(a, way, k):
        ref = shard(a, 1 - row, ring_pos(way, k), cols_2)
        return remote(ref, ref, os_.at[a, way, k], or_.at[a, way, k], (s, ring_next[way]))

    def cross(a, way, k):
        dst = shard(a, row, ring_pos(way, k), cols_1)
        return remote(owns[a].at[:, cols_1] if k == 0 else dst, dst, ys.at[a, way, k], yr.at[a, way, k], (s, beside))

    def cross_2(a):
        return remote(owns[a].at[:, cols_2], shard(a, row, z, cols_2), y2s.at[a], y2r.at[a], (s, beside))

    own_copies = [pltpu.make_async_copy(owns[a], shard(a, row, z, all_cols), own_sem.at[a]) for a in range(2)]
    for a in range(2):
        cross_2(a).start()
        for way in range(2):
            own_hop(a, way, 0).start()
        cross(a, 0, 0).start()
        own_copies[a].start()

    parity = lax.rem(z, 2)
    pairs = zn // 2

    def turn(a, line, step):
        shift = (0, 2 * parity - 1, 1 - 2 * parity, 2)[step]
        chunk = line * pairs + lax.rem(z // 2 + shift + pairs, pairs)
        span = pl.ds(pl.multiple_of(chunk * 2 * part, 2 * part), 2 * part)
        turned[a][:, span] = fulls[a][span, :].T

    def take_cross(a, k):
        for way in range(2):
            if (k > 0 or way == 0) and k <= reach[a][way]:
                wait_bytes(shard(a, 1 - row, ring_pos(way, k), cols_1), yr.at[a, way, k])

    for a in range(2):
        wait_bytes(shard(a, 1 - row, z, cols_2), y2r.at[a])
        for way in range(2):
            other_hop(a, way, 0).start()
    for a in range(2):
        own_copies[a].wait()

    for k in range(1, pairs + 1):
        for a in range(2):
            for way in range(2):
                if k <= reach[a][way]:
                    wait_bytes(shard(a, row, ring_pos(way, k), all_cols), zr.at[a, way, k - 1])
                    if k < reach[a][way]:
                        own_hop(a, way, k).start()
                    cross(a, way, k).start()
            for way in range(2):
                if k <= reach[a][way]:
                    wait_bytes(shard(a, 1 - row, ring_pos(way, k), cols_2), or_.at[a, way, k - 1])
                    if k < reach[a][way]:
                        other_hop(a, way, k).start()
        for a in range(2):
            take_cross(a, k - 1)
            turn(a, row, k - 1)
            if k > 1:
                turn(a, 1 - row, k - 2)
    for a in range(2):
        take_cross(a, pairs)
        turn(a, 1 - row, pairs - 1)

    gain_out[...] = jnp.zeros_like(gain_out)

    def incoming(i, b):
        return pl.ds(pl.multiple_of(b * rows_per, rows_per), rows_per)

    def await_from_above(i, b):
        @pl.when(not_last)
        def _():
            wait_bytes(rx.at[i, incoming(i, b)], p_recv.at[i, b])

    def give(i, b, rows, values):
        tx[i, rows] = values.astype(bf16)

        @pl.when(has_below)
        def _():
            remote(tx.at[i, rows], rx.at[i, rows], p_send.at[i], p_recv.at[i, b], (s - 1, d)).start()

    early = s < 2

    def norm_copy(a, rows):
        return remote(
            norm_full.at[a, rows, pl.ds(pl.multiple_of((1 - row) * hh, hh), hh)], norm_cat.at[a, 1, rows],
            n_send.at[a], n_recv.at[a], (s, beside),
        )

    def delta_copy(a, rows):
        return remote(
            delta_cat.at[a, 0, rows], delta_cat.at[a, 1, rows],
            d_send.at[a], d_recv.at[a], (s, beside),
        )

    def share_norm(a, b, rows, normed):
        norm_full[a, rows] = normed

        @pl.when(early)
        def _():
            norm_copy(a, rows).start()

    def share_delta(a, b, rows):
        @pl.when(early)
        def _():
            delta_copy(a, rows).start()

    first, second = pl.ds(0, h), pl.ds(h, h)

    def scale_of(values):
        return lax.rsqrt(jnp.sum(values * values, axis=-1, keepdims=True) * (1.0 / h) + offset)

    def pace(here):
        @pl.when(here)
        def _():
            pl.delay(1000)

    def upper_half(b, carry):
        rows = pl.ds(pl.multiple_of(b * rows_per, rows_per), rows_per)
        gain_f, gain_g = gains_ref[0:1, :], gains_ref[1:2, :]
        pace(jnp.logical_and(is_last, b > 0))
        await_from_above(1, b)
        await_from_above(0, b)
        y1 = jnp.where(is_last, pair_ref[rows, first], rx[0, rows].astype(f32))
        y2 = jnp.where(is_last, pair_ref[rows, second], rx[1, rows].astype(f32))
        y1s[rows] = y1
        r1 = scale_of(y1)
        pre_g = jnp.dot((y1 * gain_g).astype(bf16), wg[...], preferred_element_type=f32) * r1
        sig_g = jax.nn.sigmoid(pre_g)
        x2 = y2 - pre_g * sig_g
        give(1, b, rows, x2)
        r2 = scale_of(x2)
        pre_f = jnp.dot((x2 * gain_f).astype(bf16), wf[...], preferred_element_type=f32) * r2
        sig_f = jax.nn.sigmoid(pre_f)
        x1 = y1 - pre_f * sig_f
        give(0, b, rows, x1)
        in_pair_ref[rows, first] = x1
        in_pair_ref[rows, second] = x2
        pres[0, rows] = pre_g
        pres[1, rows] = pre_f
        slopes[0, rows] = sig_g * (1.0 + pre_g * (1.0 - sig_g))
        slopes[1, rows] = sig_f * (1.0 + pre_f * (1.0 - sig_f))
        share_norm(0, b, rows, (y1 * r1 * gain_g).astype(bf16))
        share_norm(1, b, rows, (x2 * r2 * gain_f).astype(bf16))

        return carry

    def lower_half(b, carry):
        rows = pl.ds(pl.multiple_of(b * rows_per, rows_per), rows_per)
        gain_f, gain_g = gains_ref[0:1, :], gains_ref[1:2, :]
        pace(is_last)
        await_from_above(2, b)
        await_from_above(3, b)
        gy1 = jnp.where(is_last, grad_ref[rows, first].astype(f32), rx[2, rows].astype(f32))
        gy2 = jnp.where(is_last, grad_ref[rows, second].astype(f32), rx[3, rows].astype(f32))
        delta_g = (gy2 * slopes[0, rows]).astype(bf16)
        back_g = jnp.dot(delta_g, wgt[...], preferred_element_type=f32)
        mean_g = jnp.sum(delta_g.astype(f32) * pres[0, rows], axis=-1, keepdims=True) * (1.0 / h)
        y1 = y1s[rows]
        r1 = scale_of(y1)
        gz = gy1 + (r1 * gain_g) * back_g - y1 * (mean_g * (r1 * r1))
        give(2, b, rows, gz)
        delta_f = (gz * slopes[1, rows]).astype(bf16)
        back_f = jnp.dot(delta_f, wft[...], preferred_element_type=f32)
        mean_f = jnp.sum(delta_f.astype(f32) * pres[1, rows], axis=-1, keepdims=True) * (1.0 / h)
        x2 = in_pair_ref[rows, second]
        r2 = scale_of(x2)
        gx2 = gy2 + (r2 * gain_f) * back_f - x2 * (mean_f * (r2 * r2))
        give(3, b, rows, gx2)
        in_grad_ref[rows, first] = gz.astype(bf16)
        in_grad_ref[rows, second] = gx2.astype(bf16)
        delta_cat[0, 0, rows] = delta_g
        delta_cat[1, 0, rows] = delta_f
        share_delta(0, b, rows)
        share_delta(1, b, rows)
        gain_out[1:2, :] += jnp.sum(back_g * (y1 * r1), axis=0, keepdims=True)
        gain_out[0:1, :] += jnp.sum(back_f * (x2 * r2), axis=0, keepdims=True)
        return carry

    lax.fori_loop(0, blocks, upper_half, 0)
    lax.fori_loop(0, blocks, lower_half, 0)

    @pl.when(has_below)
    def _():
        for i in range(4):
            wait_bytes(tx.at[i], p_send.at[i])

    upper = lax.rem(s, 2) == 1

    @pl.when(jnp.logical_not(early))
    def _():
        @pl.when(jnp.logical_not(upper))
        def _():
            pl.semaphore_signal(turn_sem, inc=1, device_id=(s + 1, d), device_id_type=MESH)

        @pl.when(upper)
        def _():
            pl.semaphore_wait(turn_sem, 1)

        for a in range(2):
            norm_copy(a, pl.ds(0, tokens)).start()
            delta_copy(a, pl.ds(0, tokens)).start()

    gain_parts[d] = gain_out[...]
    for k in range(1, n):
        remote(gain_parts.at[d], gain_parts.at[d], c_send, c_recv, (s, lax.rem(d + k, n))).start()

    for a in range(2):
        norm_cat[a, 0] = norm_full[a, :, pl.ds(pl.multiple_of(row * hh, hh), hh)]

    def slot(pos):
        return pl.ds(pl.multiple_of(pos * part, part), part)

    def sum_hop(a, way, t):
        return remote(rs_tx.at[a, way, t], rs_rx.at[a, way, t], r_send.at[a, way, t], r_recv.at[a, way, t], (s, ring_next[way]))

    def sum_pos(a, way, t):
        far = reach[a][way] - t
        return lax.rem(z + (far if way == 0 else zn - far), zn)

    for a in range(2):
        wait_bytes(norm_cat.at[a, 1], n_recv.at[a])
        wait_bytes(delta_cat.at[a, 1], d_recv.at[a])
        sums[a] = lax.dot_general(
            norm_cat[a].reshape(2 * tokens, hh), delta_cat[a].reshape(2 * tokens, h),
            (((0,), (0,)), ((), ())), preferred_element_type=f32,
        )
        for way in range(2):
            if reach[a][way] > 0:
                rs_tx[a, way, 0] = sums[a, slot(sum_pos(a, way, 0))].astype(bf16)
                sum_hop(a, way, 0).start()
    for t in range(1, pairs):
        for a in range(2):
            for way in range(2):
                if t < reach[a][way]:
                    wait_bytes(rs_rx.at[a, way, t - 1], r_recv.at[a, way, t - 1])
                    rs_tx[a, way, t] = (sums[a, slot(sum_pos(a, way, t))] + rs_rx[a, way, t - 1].astype(f32)).astype(bf16)
                    sum_hop(a, way, t).start()
    for a, out in ((0, g_out), (1, f_out)):
        total = sums[a, slot(z)]
        for way in range(2):
            if reach[a][way] > 0:
                last = reach[a][way] - 1
                wait_bytes(rs_rx.at[a, way, last], r_recv.at[a, way, last])
                total = total + rs_rx[a, way, last].astype(f32)
        out[...] = total

    others = pl.ds(0, n - 1)
    wait_bytes(gain_parts.at[others], c_recv)
    total = gain_parts[0]
    for e in range(1, n):
        total = total + gain_parts[e]
    gain_out[...] = total

    wait_bytes(gain_parts.at[others], c_send)
    for a in range(2):
        wait_bytes(norm_cat.at[a, 1], n_send.at[a])
        wait_bytes(delta_cat.at[a, 1], d_send.at[a])
        cross_2(a).wait_send()
        cross(a, 0, 0).wait_send()
        for way in range(2):
            for k in range(reach[a][way]):
                own_hop(a, way, k).wait_send()
                other_hop(a, way, k).wait_send()
                cross(a, way, k + 1).wait_send()
                sum_hop(a, way, k).wait_send()


def hand_over(*refs):
    n = (len(refs) - 2) // 3
    ins, outs, held, in_sem, out_sem = refs[:n], refs[n:2 * n], refs[2 * n:3 * n], refs[-2], refs[-1]
    loads = [pltpu.make_async_copy(ins[i], held[i], in_sem.at[i]) for i in range(n)]
    stores = [pltpu.make_async_copy(held[i], outs[i].at[0], out_sem.at[i]) for i in range(n)]
    for copy in loads:
        copy.start()
    for load, store in zip(loads, stores):
        load.wait()
        store.start()
    for copy in stores:
        copy.wait()


def shards(out_pair, out_grad, f_weight, g_weight, gains):
    n, sections = lax.axis_size("dp"), lax.axis_size("section")
    tokens, width = out_pair.shape
    h = width // 2
    part = f_weight.shape[1]
    blocks = 8
    zn = n // 2
    hops = max(zn // 2, 1)
    vmem = pl.BlockSpec(memory_space=pltpu.VMEM)
    dma = pltpu.SemaphoreType.DMA
    outs = pl.pallas_call(
        functools.partial(kernel, n, sections, blocks),
        out_shape=(
            jax.ShapeDtypeStruct((tokens, width), f32),
            jax.ShapeDtypeStruct((tokens, width), bf16),
            jax.ShapeDtypeStruct((part, h), f32),
            jax.ShapeDtypeStruct((part, h), f32),
            jax.ShapeDtypeStruct((2, h), f32),
        ),
        in_specs=[vmem] * 5,
        out_specs=[vmem] * 5,
        scratch_shapes=[
            pltpu.VMEM((h, h), bf16),
            pltpu.VMEM((h, h), bf16),
            pltpu.VMEM((h, h), bf16),
            pltpu.VMEM((h, h), bf16),
            pltpu.VMEM((4, tokens, h), bf16),
            pltpu.VMEM((4, tokens, h), bf16),
            pltpu.VMEM((tokens, h), f32),
            pltpu.VMEM((2, tokens, h), f32),
            pltpu.VMEM((2, tokens, h), f32),
            pltpu.VMEM((2, tokens, h), bf16),
            pltpu.VMEM((2, 2, tokens, zn * part), bf16),
            pltpu.VMEM((2, 2, tokens, h), bf16),
            pltpu.VMEM((2, zn * part, h), f32),
            pltpu.VMEM((2, 2, hops, part, h), bf16),
            pltpu.VMEM((2, 2, hops, part, h), bf16),
            pltpu.VMEM((n, 2, h), f32),
            dma((2,)),
            dma((2, 2, hops)),
            dma((2, 2, hops)),
            dma((2, 2, hops)),
            dma((2, 2, hops)),
            dma((2, 2, hops + 1)),
            dma((2, 2, hops + 1)),
            dma((2,)),
            dma((2,)),
            dma((4,)),
            dma((4, blocks)),
            dma((2,)),
            dma((2,)),
            dma((2,)),
            dma((2,)),
            dma((2, 2, hops)),
            dma((2, 2, hops)),
            dma,
            dma,
            pltpu.SemaphoreType.REGULAR,
        ],
        compiler_params=pltpu.CompilerParams(
            collective_id=0, has_side_effects=True, vmem_limit_bytes=60 * 1024 * 1024
        ),
    )(out_pair, out_grad, f_weight[0], g_weight[0], gains[0])
    count = len(outs)
    return pl.pallas_call(
        hand_over,
        out_shape=tuple(jax.ShapeDtypeStruct((1,) + out.shape, out.dtype) for out in outs),
        in_specs=[pl.BlockSpec(memory_space=pl.ANY)] * count,
        out_specs=tuple([pl.BlockSpec(memory_space=pl.ANY)] * count),
        scratch_shapes=[pltpu.VMEM(out.shape, out.dtype) for out in outs] + [dma((count,)), dma((count,))],
    )(*outs)


def solution(mesh):
    placed = (
        P("dp", None),
        P("dp", None),
        P("section", "dp", None),
        P("section", "dp", None),
        P("section", None, None),
    )
    return jax.shard_map(
        shards,
        mesh=mesh,
        in_specs=placed,
        out_specs=(
            P("section", "dp", None),
            P("section", "dp", None),
            P("section", "dp", None),
            P("section", "dp", None),
            P("section", None, None),
        ),
        check_vma=False,
    )
```

```python
import functools

import jax
import jax.numpy as jnp
from jax import lax
from jax.experimental import pallas as pl
from jax.experimental.pallas import tpu as pltpu
from jax.sharding import PartitionSpec as P

offset = 0.25
MESH = pl.DeviceIdType.MESH
f32, bf16 = jnp.float32, jnp.bfloat16


def kernel(
    n, sections, blocks, cuts,
    pair_ref, grad_ref, fw_ref, gw_ref, gains_ref,
    in_pair_ref, in_grad_ref, f_out, g_out, gain_out,
    wf, wg, wft, wgt, rx, tx, y1s, pres, slopes, norm_full, norm_cat, delta_cat, sums, norm_turned, rs_rx, rs_tx, res_tx, res_rx, gain_parts,
    own_sem, zs, zr, os_, or_, ys, yr, y2s, y2r, p_send, p_recv, n_send, n_recv, d_send, d_recv, r_send, r_recv, c_send, c_recv, turn_sem, nl_send, nl_recv, dl_send, dl_recv, s_send, s_recv,
):
    s, d = lax.axis_index("section"), lax.axis_index("dp")
    is_last = s == sections - 1
    has_below = s > 0
    not_last = jnp.logical_not(is_last)
    tokens = pair_ref.shape[0]
    h = pair_ref.shape[1] // 2
    part = fw_ref.shape[0]
    rows_per = tokens // blocks
    zn = n // 2
    hh = zn * part
    z, row = lax.rem(d, zn), d // zn
    beside = (1 - row) * zn + z
    ring_next = (row * zn + lax.rem(z + 1, zn), row * zn + lax.rem(z + zn - 1, zn))

    barrier = pltpu.get_barrier_semaphore()
    for k in range(1, n):
        pl.semaphore_signal(barrier, inc=1, device_id=(s, lax.rem(d + k, n)), device_id_type=MESH)

    @pl.when(has_below)
    def _():
        pl.semaphore_signal(barrier, inc=1, device_id=(s - 1, d), device_id_type=MESH)

    @pl.when(not_last)
    def _():
        pl.semaphore_signal(barrier, inc=1, device_id=(s + 1, d), device_id_type=MESH)

    client, proxy = 1, 1 + sections * 3 // 4
    is_client, is_proxy = s == client, s == proxy

    @pl.when(is_client)
    def _():
        pl.semaphore_signal(barrier, inc=1, device_id=(proxy, d), device_id_type=MESH)

    @pl.when(is_proxy)
    def _():
        pl.semaphore_signal(barrier, inc=1, device_id=(client, d), device_id_type=MESH)

    linked = jnp.logical_or(is_client, is_proxy).astype(jnp.int32)
    pl.semaphore_wait(barrier, n - 1 + has_below.astype(jnp.int32) + not_last.astype(jnp.int32) + linked)

    def remote(src, dst, send, recv, target):
        return pltpu.make_async_remote_copy(
            src_ref=src, dst_ref=dst, send_sem=send, recv_sem=recv,
            device_id=target, device_id_type=MESH,
        )

    def wait_bytes(ref, sem):
        pltpu.make_async_copy(ref, ref, sem).wait()

    fulls, owns, turned = (wg, wf), (gw_ref, fw_ref), (wgt, wft)
    c1 = h * 5 // 8
    cols_1, cols_2, all_cols = pl.ds(0, c1), pl.ds(c1, h - c1), pl.ds(0, h)
    reach = ((zn // 2, zn - 1 - zn // 2), (zn - 1 - zn // 2, zn // 2))

    def ring_pos(way, k):
        return lax.rem(z + (zn - k if way == 0 else k), zn)

    def shard(a, line, pos, cols):
        return fulls[a].at[pl.ds(pl.multiple_of((line * zn + pos) * part, part), part), cols]

    def own_hop(a, way, k):
        dst = shard(a, row, ring_pos(way, k), all_cols)
        return remote(owns[a] if k == 0 else dst, dst, zs.at[a, way, k], zr.at[a, way, k], (s, ring_next[way]))

    def other_hop(a, way, k):
        ref = shard(a, 1 - row, ring_pos(way, k), cols_2)
        return remote(ref, ref, os_.at[a, way, k], or_.at[a, way, k], (s, ring_next[way]))

    def cross(a, way, k):
        dst = shard(a, row, ring_pos(way, k), cols_1)
        return remote(owns[a].at[:, cols_1] if k == 0 else dst, dst, ys.at[a, way, k], yr.at[a, way, k], (s, beside))

    def cross_2(a):
        return remote(owns[a].at[:, cols_2], shard(a, row, z, cols_2), y2s.at[a], y2r.at[a], (s, beside))

    own_copies = [pltpu.make_async_copy(owns[a], shard(a, row, z, all_cols), own_sem.at[a]) for a in range(2)]
    for a in range(2):
        cross_2(a).start()
        for way in range(2):
            own_hop(a, way, 0).start()
        cross(a, 0, 0).start()
        own_copies[a].start()

    parity = lax.rem(z, 2)
    pairs = zn // 2

    def turn(a, line, step):
        shift = (0, 2 * parity - 1, 1 - 2 * parity, 2)[step]
        chunk = line * pairs + lax.rem(z // 2 + shift + pairs, pairs)
        span = pl.ds(pl.multiple_of(chunk * 2 * part, 2 * part), 2 * part)
        turned[a][:, span] = fulls[a][span, :].T

    def take_cross(a, k):
        for way in range(2):
            if (k > 0 or way == 0) and k <= reach[a][way]:
                wait_bytes(shard(a, 1 - row, ring_pos(way, k), cols_1), yr.at[a, way, k])

    for a in range(2):
        wait_bytes(shard(a, 1 - row, z, cols_2), y2r.at[a])
        for way in range(2):
            other_hop(a, way, 0).start()
    for a in range(2):
        own_copies[a].wait()

    for k in range(1, pairs + 1):
        for a in range(2):
            for way in range(2):
                if k <= reach[a][way]:
                    wait_bytes(shard(a, row, ring_pos(way, k), all_cols), zr.at[a, way, k - 1])
                    if k < reach[a][way]:
                        own_hop(a, way, k).start()
                    cross(a, way, k).start()
            for way in range(2):
                if k <= reach[a][way]:
                    wait_bytes(shard(a, 1 - row, ring_pos(way, k), cols_2), or_.at[a, way, k - 1])
                    if k < reach[a][way]:
                        other_hop(a, way, k).start()
        for a in range(2):
            take_cross(a, k - 1)
            turn(a, row, k - 1)
            if k > 1:
                turn(a, 1 - row, k - 2)
    for a in range(2):
        take_cross(a, pairs)
        turn(a, 1 - row, pairs - 1)

    gain_out[...] = jnp.zeros_like(gain_out)

    def incoming(i, b):
        return pl.ds(pl.multiple_of(b * rows_per, rows_per), rows_per)

    def await_from_above(i, b):
        @pl.when(not_last)
        def _():
            wait_bytes(rx.at[i, incoming(i, b)], p_recv.at[i, b])

    def give(i, b, rows, values):
        tx[i, rows] = values.astype(bf16)

        @pl.when(has_below)
        def _():
            remote(tx.at[i, rows], rx.at[i, rows], p_send.at[i], p_recv.at[i, b], (s - 1, d)).start()

    streams = jnp.logical_and(s < 4, jnp.logical_not(is_client))
    away = pl.ds(pl.multiple_of((1 - row) * hh, hh), hh)

    def norm_copy(q, a, rows):
        return remote(
            norm_full.at[q, a, rows, away], norm_cat.at[q, a, 1, rows],
            n_send.at[q, a], n_recv.at[q, a], (s, beside),
        )

    def delta_copy(q, a, rows):
        return remote(
            delta_cat.at[q, a, 0, rows], delta_cat.at[q, a, 1, rows],
            d_send.at[q, a], d_recv.at[q, a], (s, beside),
        )

    def norm_lend(a, b, rows):
        return remote(norm_full.at[0, a, rows], norm_full.at[1, a, rows], nl_send.at[a], nl_recv.at[a, b], (proxy, d))

    def delta_lend(a, b, rows):
        return remote(
            delta_cat.at[0, a, 0, rows], delta_cat.at[1, a, 0, rows], dl_send.at[a], dl_recv.at[a, b], (proxy, d)
        )

    def share_norm(a, b, rows, normed):
        norm_full[0, a, rows] = normed

        @pl.when(streams)
        def _():
            norm_copy(0, a, rows).start()

        @pl.when(is_client)
        def _():
            norm_lend(a, b, rows).start()

    def share_delta(a, b, rows):
        @pl.when(streams)
        def _():
            delta_copy(0, a, rows).start()

        @pl.when(is_client)
        def _():
            delta_lend(a, b, rows).start()

    first, second = pl.ds(0, h), pl.ds(h, h)

    def scale_of(values):
        return lax.rsqrt(jnp.sum(values * values, axis=-1, keepdims=True) * (1.0 / h) + offset)

    def pace(here):
        @pl.when(here)
        def _():
            pl.delay(1000)

    def upper_half(b, carry):
        rows = pl.ds(pl.multiple_of(b * rows_per, rows_per), rows_per)
        gain_f, gain_g = gains_ref[0:1, :], gains_ref[1:2, :]
        pace(jnp.logical_and(is_last, b > 0))
        await_from_above(1, b)
        await_from_above(0, b)
        y1 = jnp.where(is_last, pair_ref[rows, first], rx[0, rows].astype(f32))
        y2 = jnp.where(is_last, pair_ref[rows, second], rx[1, rows].astype(f32))
        y1s[rows] = y1
        r1 = scale_of(y1)
        pre_g = jnp.dot((y1 * gain_g).astype(bf16), wg[...], preferred_element_type=f32) * r1
        sig_g = jax.nn.sigmoid(pre_g)
        x2 = y2 - pre_g * sig_g
        give(1, b, rows, x2)
        r2 = scale_of(x2)
        pre_f = jnp.dot((x2 * gain_f).astype(bf16), wf[...], preferred_element_type=f32) * r2
        sig_f = jax.nn.sigmoid(pre_f)
        x1 = y1 - pre_f * sig_f
        give(0, b, rows, x1)
        in_pair_ref[rows, first] = x1
        in_pair_ref[rows, second] = x2
        pres[0, rows] = pre_g
        pres[1, rows] = pre_f
        slopes[0, rows] = sig_g * (1.0 + pre_g * (1.0 - sig_g))
        slopes[1, rows] = sig_f * (1.0 + pre_f * (1.0 - sig_f))
        share_norm(0, b, rows, (y1 * r1 * gain_g).astype(bf16))
        share_norm(1, b, rows, (x2 * r2 * gain_f).astype(bf16))

        return carry

    def lower_half(b, carry):
        rows = pl.ds(pl.multiple_of(b * rows_per, rows_per), rows_per)
        gain_f, gain_g = gains_ref[0:1, :], gains_ref[1:2, :]
        pace(is_last)
        await_from_above(2, b)
        await_from_above(3, b)
        gy1 = jnp.where(is_last, grad_ref[rows, first].astype(f32), rx[2, rows].astype(f32))
        gy2 = jnp.where(is_last, grad_ref[rows, second].astype(f32), rx[3, rows].astype(f32))
        delta_g = (gy2 * slopes[0, rows]).astype(bf16)
        back_g = jnp.dot(delta_g, wgt[...], preferred_element_type=f32)
        mean_g = jnp.sum(delta_g.astype(f32) * pres[0, rows], axis=-1, keepdims=True) * (1.0 / h)
        y1 = y1s[rows]
        r1 = scale_of(y1)
        gz = gy1 + (r1 * gain_g) * back_g - y1 * (mean_g * (r1 * r1))
        give(2, b, rows, gz)
        delta_f = (gz * slopes[1, rows]).astype(bf16)
        back_f = jnp.dot(delta_f, wft[...], preferred_element_type=f32)
        mean_f = jnp.sum(delta_f.astype(f32) * pres[1, rows], axis=-1, keepdims=True) * (1.0 / h)
        x2 = in_pair_ref[rows, second]
        r2 = scale_of(x2)
        gx2 = gy2 + (r2 * gain_f) * back_f - x2 * (mean_f * (r2 * r2))
        give(3, b, rows, gx2)
        in_grad_ref[rows, first] = gz.astype(bf16)
        in_grad_ref[rows, second] = gx2.astype(bf16)
        delta_cat[0, 0, 0, rows] = delta_g
        delta_cat[0, 1, 0, rows] = delta_f
        share_delta(0, b, rows)
        share_delta(1, b, rows)
        gain_out[1:2, :] += jnp.sum(back_g * (y1 * r1), axis=0, keepdims=True)
        gain_out[0:1, :] += jnp.sum(back_f * (x2 * r2), axis=0, keepdims=True)
        return carry

    lax.fori_loop(0, blocks, upper_half, 0)
    lax.fori_loop(0, blocks, lower_half, 0)

    @pl.when(has_below)
    def _():
        for i in range(4):
            wait_bytes(tx.at[i], p_send.at[i])

    upper = lax.rem(s, 2) == 1

    @pl.when(s >= 4)
    def _():
        @pl.when(jnp.logical_not(upper))
        def _():
            pl.semaphore_signal(turn_sem, inc=1, device_id=(s + 1, d), device_id_type=MESH)

        @pl.when(upper)
        def _():
            pl.semaphore_wait(turn_sem, 1)

        for a in range(2):
            norm_copy(0, a, pl.ds(0, tokens)).start()
            delta_copy(0, a, pl.ds(0, tokens)).start()

    gain_parts[d] = gain_out[...]
    for k in range(1, n):
        remote(gain_parts.at[d], gain_parts.at[d], c_send, c_recv, (s, lax.rem(d + k, n))).start()

    def slot(pos):
        return pl.ds(pl.multiple_of(pos * part, part), part)

    def sum_hop(q, a, way, t, c):
        return remote(
            rs_tx.at[q, a, way, t, c], rs_rx.at[q, a, way, t, c],
            r_send.at[q, a, way, t, c], r_recv.at[q, a, way, t, c], (s, ring_next[way]),
        )

    span = h // cuts

    def band(c):
        return pl.ds(c * span, span)

    def sum_pos(a, way, t):
        far = reach[a][way] - t
        return lax.rem(z + (far if way == 0 else zn - far), zn)

    def reduce_grads(q, emit):
        for a in range(2):
            wait_bytes(norm_cat.at[q, a, 1], n_recv.at[q, a])
            norm_cat[q, a, 0] = norm_full[q, a, :, pl.ds(pl.multiple_of(row * hh, hh), hh)]
            norm_turned[a] = norm_cat[q, a].reshape(2 * tokens, hh).T
        for a in range(2):
            wait_bytes(delta_cat.at[q, a, 1], d_recv.at[q, a])
            for c in range(cuts):
                sums[a, :, band(c)] = jnp.dot(
                    norm_turned[a], delta_cat[q, a, :, :, band(c)].reshape(2 * tokens, span), preferred_element_type=f32
                )
                for way in range(2):
                    if reach[a][way] > 0:
                        rs_tx[q, a, way, 0, c] = sums[a, slot(sum_pos(a, way, 0)), band(c)].astype(bf16)
                        sum_hop(q, a, way, 0, c).start()
        for t in range(1, pairs):
            for a in range(2):
                for c in range(cuts):
                    for way in range(2):
                        if t < reach[a][way]:
                            wait_bytes(rs_rx.at[q, a, way, t - 1, c], r_recv.at[q, a, way, t - 1, c])
                            rs_tx[q, a, way, t, c] = (
                                sums[a, slot(sum_pos(a, way, t)), band(c)] + rs_rx[q, a, way, t - 1, c].astype(f32)
                            ).astype(bf16)
                            sum_hop(q, a, way, t, c).start()
        for a in range(2):
            for c in range(cuts):
                total = sums[a, slot(z), band(c)]
                for way in range(2):
                    if reach[a][way] > 0:
                        last = reach[a][way] - 1
                        wait_bytes(rs_rx.at[q, a, way, last, c], r_recv.at[q, a, way, last, c])
                        total = total + rs_rx[q, a, way, last, c].astype(f32)
                emit(a, c, total)
        for a in range(2):
            wait_bytes(norm_cat.at[q, a, 1], n_send.at[q, a])
            wait_bytes(delta_cat.at[q, a, 1], d_send.at[q, a])
            for way in range(2):
                for k in range(reach[a][way]):
                    for c in range(cuts):
                        sum_hop(q, a, way, k, c).wait_send()

    grads = (g_out, f_out)

    def keep(a, c, total):
        grads[a][:, band(c)] = total

    def give_back(a, c):
        return remote(res_tx.at[a, c], res_rx.at[a, c], s_send.at[a, c], s_recv.at[a, c], (client, d))

    def lend_back(a, c, total):
        res_tx[a, c] = total.astype(bf16)
        give_back(a, c).start()

    @pl.when(jnp.logical_not(is_client))
    def _():
        reduce_grads(0, keep)

    @pl.when(is_proxy)
    def _():
        def lent_norms(b, carry):
            rows = pl.ds(pl.multiple_of(b * rows_per, rows_per), rows_per)
            for a in range(2):
                wait_bytes(norm_full.at[1, a, rows], nl_recv.at[a, b])
                norm_copy(1, a, rows).start()
            return carry

        def lent_deltas(b, carry):
            rows = pl.ds(pl.multiple_of(b * rows_per, rows_per), rows_per)
            for a in range(2):
                wait_bytes(delta_cat.at[1, a, 0, rows], dl_recv.at[a, b])
                delta_copy(1, a, rows).start()
            return carry

        lax.fori_loop(0, blocks, lent_norms, 0)
        lax.fori_loop(0, blocks, lent_deltas, 0)
        reduce_grads(1, lend_back)
        for a in range(2):
            for c in range(cuts):
                give_back(a, c).wait_send()

    @pl.when(is_client)
    def _():
        for a in range(2):
            for c in range(cuts):
                wait_bytes(res_rx.at[a, c], s_recv.at[a, c])
                grads[a][:, band(c)] = res_rx[a, c].astype(f32)
        for a in range(2):
            wait_bytes(norm_full.at[0, a], nl_send.at[a])
            wait_bytes(delta_cat.at[0, a, 0], dl_send.at[a])

    others = pl.ds(0, n - 1)
    wait_bytes(gain_parts.at[others], c_recv)
    total = gain_parts[0]
    for e in range(1, n):
        total = total + gain_parts[e]
    gain_out[...] = total

    wait_bytes(gain_parts.at[others], c_send)
    for a in range(2):
        cross_2(a).wait_send()
        cross(a, 0, 0).wait_send()
        for way in range(2):
            for k in range(reach[a][way]):
                own_hop(a, way, k).wait_send()
                other_hop(a, way, k).wait_send()
                cross(a, way, k + 1).wait_send()


def hand_over(*refs):
    n = (len(refs) - 2) // 3
    ins, outs, held, in_sem, out_sem = refs[:n], refs[n:2 * n], refs[2 * n:3 * n], refs[-2], refs[-1]
    loads = [pltpu.make_async_copy(ins[i], held[i], in_sem.at[i]) for i in range(n)]
    stores = [pltpu.make_async_copy(held[i], outs[i].at[0], out_sem.at[i]) for i in range(n)]
    for copy in loads:
        copy.start()
    for load, store in zip(loads, stores):
        load.wait()
        store.start()
    for copy in stores:
        copy.wait()


def shards(out_pair, out_grad, f_weight, g_weight, gains):
    n, sections = lax.axis_size("dp"), lax.axis_size("section")
    tokens, width = out_pair.shape
    h = width // 2
    part = f_weight.shape[1]
    blocks, cuts = 8, 2
    zn = n // 2
    hops = max(zn // 2, 1)
    vmem = pl.BlockSpec(memory_space=pltpu.VMEM)
    dma = pltpu.SemaphoreType.DMA
    outs = pl.pallas_call(
        functools.partial(kernel, n, sections, blocks, cuts),
        out_shape=(
            jax.ShapeDtypeStruct((tokens, width), f32),
            jax.ShapeDtypeStruct((tokens, width), bf16),
            jax.ShapeDtypeStruct((part, h), f32),
            jax.ShapeDtypeStruct((part, h), f32),
            jax.ShapeDtypeStruct((2, h), f32),
        ),
        in_specs=[vmem] * 5,
        out_specs=[vmem] * 5,
        scratch_shapes=[
            pltpu.VMEM((h, h), bf16),
            pltpu.VMEM((h, h), bf16),
            pltpu.VMEM((h, h), bf16),
            pltpu.VMEM((h, h), bf16),
            pltpu.VMEM((4, tokens, h), bf16),
            pltpu.VMEM((4, tokens, h), bf16),
            pltpu.VMEM((tokens, h), f32),
            pltpu.VMEM((2, tokens, h), f32),
            pltpu.VMEM((2, tokens, h), f32),
            pltpu.VMEM((2, 2, tokens, h), bf16),
            pltpu.VMEM((2, 2, 2, tokens, zn * part), bf16),
            pltpu.VMEM((2, 2, 2, tokens, h), bf16),
            pltpu.VMEM((2, zn * part, h), f32),
            pltpu.VMEM((2, zn * part, 2 * tokens), bf16),
            pltpu.VMEM((2, 2, 2, hops, cuts, part, h // cuts), bf16),
            pltpu.VMEM((2, 2, 2, hops, cuts, part, h // cuts), bf16),
            pltpu.VMEM((2, cuts, part, h // cuts), bf16),
            pltpu.VMEM((2, cuts, part, h // cuts), bf16),
            pltpu.VMEM((n, 2, h), f32),
            dma((2,)),
            dma((2, 2, hops)),
            dma((2, 2, hops)),
            dma((2, 2, hops)),
            dma((2, 2, hops)),
            dma((2, 2, hops + 1)),
            dma((2, 2, hops + 1)),
            dma((2,)),
            dma((2,)),
            dma((4,)),
            dma((4, blocks)),
            dma((2, 2)),
            dma((2, 2)),
            dma((2, 2)),
            dma((2, 2)),
            dma((2, 2, 2, hops, cuts)),
            dma((2, 2, 2, hops, cuts)),
            dma,
            dma,
            pltpu.SemaphoreType.REGULAR,
            dma((2,)),
            dma((2, blocks)),
            dma((2,)),
            dma((2, blocks)),
            dma((2, cuts)),
            dma((2, cuts)),
        ],
        compiler_params=pltpu.CompilerParams(
            collective_id=0, has_side_effects=True, vmem_limit_bytes=60 * 1024 * 1024
        ),
    )(out_pair, out_grad, f_weight[0], g_weight[0], gains[0])
    count = len(outs)
    return pl.pallas_call(
        hand_over,
        out_shape=tuple(jax.ShapeDtypeStruct((1,) + out.shape, out.dtype) for out in outs),
        in_specs=[pl.BlockSpec(memory_space=pl.ANY)] * count,
        out_specs=tuple([pl.BlockSpec(memory_space=pl.ANY)] * count),
        scratch_shapes=[pltpu.VMEM(out.shape, out.dtype) for out in outs] + [dma((count,)), dma((count,))],
    )(*outs)


def solution(mesh):
    placed = (
        P("dp", None),
        P("dp", None),
        P("section", "dp", None),
        P("section", "dp", None),
        P("section", None, None),
    )
    return jax.shard_map(
        shards,
        mesh=mesh,
        in_specs=placed,
        out_specs=(
            P("section", "dp", None),
            P("section", "dp", None),
            P("section", "dp", None),
            P("section", "dp", None),
            P("section", None, None),
        ),
        check_vma=False,
    )
```

```python
import functools

import jax
import jax.numpy as jnp
from jax import lax
from jax.experimental import pallas as pl
from jax.experimental.pallas import tpu as pltpu
from jax.sharding import PartitionSpec as P

offset = 0.25
MESH = pl.DeviceIdType.MESH
f32, bf16 = jnp.float32, jnp.bfloat16


def kernel(
    n, sections, blocks, cuts,
    pair_ref, grad_ref, fw_ref, gw_ref, gains_ref,
    in_pair_ref, in_grad_ref, f_out, g_out, gain_out,
    wf, wg, wft, wgt, rx, tx, y1s, pres, slopes, norm_full, norm_cat, delta_cat, sums, norm_turned, rs_rx, rs_tx, res_tx, res_rx, gain_parts,
    own_sem, zs, zr, os_, or_, ys, yr, y2s, y2r, p_send, p_recv, n_send, n_recv, d_send, d_recv, r_send, r_recv, c_send, c_recv, turn_sem, nl_send, nl_recv, dl_send, dl_recv, s_send, s_recv,
):
    s, d = lax.axis_index("section"), lax.axis_index("dp")
    is_last = s == sections - 1
    has_below = s > 0
    not_last = jnp.logical_not(is_last)
    tokens = pair_ref.shape[0]
    h = pair_ref.shape[1] // 2
    part = fw_ref.shape[0]
    rows_per = tokens // blocks
    zn = n // 2
    hh = zn * part
    z, row = lax.rem(d, zn), d // zn
    beside = (1 - row) * zn + z
    ring_next = (row * zn + lax.rem(z + 1, zn), row * zn + lax.rem(z + zn - 1, zn))

    barrier = pltpu.get_barrier_semaphore()
    for k in range(1, n):
        pl.semaphore_signal(barrier, inc=1, device_id=(s, lax.rem(d + k, n)), device_id_type=MESH)

    @pl.when(has_below)
    def _():
        pl.semaphore_signal(barrier, inc=1, device_id=(s - 1, d), device_id_type=MESH)

    @pl.when(not_last)
    def _():
        pl.semaphore_signal(barrier, inc=1, device_id=(s + 1, d), device_id_type=MESH)

    client, proxy = 1, 1 + sections * 3 // 4
    is_client, is_proxy = s == client, s == proxy

    @pl.when(is_client)
    def _():
        pl.semaphore_signal(barrier, inc=1, device_id=(proxy, d), device_id_type=MESH)

    @pl.when(is_proxy)
    def _():
        pl.semaphore_signal(barrier, inc=1, device_id=(client, d), device_id_type=MESH)

    linked = jnp.logical_or(is_client, is_proxy).astype(jnp.int32)
    pl.semaphore_wait(barrier, n - 1 + has_below.astype(jnp.int32) + not_last.astype(jnp.int32) + linked)

    def remote(src, dst, send, recv, target):
        return pltpu.make_async_remote_copy(
            src_ref=src, dst_ref=dst, send_sem=send, recv_sem=recv,
            device_id=target, device_id_type=MESH,
        )

    def wait_bytes(ref, sem):
        pltpu.make_async_copy(ref, ref, sem).wait()

    fulls, owns, turned = (wg, wf), (gw_ref, fw_ref), (wgt, wft)
    c1 = h * 5 // 8
    cols_1, cols_2, all_cols = pl.ds(0, c1), pl.ds(c1, h - c1), pl.ds(0, h)
    reach = ((zn // 2, zn - 1 - zn // 2), (zn - 1 - zn // 2, zn // 2))

    def ring_pos(way, k):
        return lax.rem(z + (zn - k if way == 0 else k), zn)

    def shard(a, line, pos, cols):
        return fulls[a].at[pl.ds(pl.multiple_of((line * zn + pos) * part, part), part), cols]

    def own_hop(a, way, k):
        dst = shard(a, row, ring_pos(way, k), all_cols)
        return remote(owns[a] if k == 0 else dst, dst, zs.at[a, way, k], zr.at[a, way, k], (s, ring_next[way]))

    def other_hop(a, way, k):
        ref = shard(a, 1 - row, ring_pos(way, k), cols_2)
        return remote(ref, ref, os_.at[a, way, k], or_.at[a, way, k], (s, ring_next[way]))

    def cross(a, way, k):
        dst = shard(a, row, ring_pos(way, k), cols_1)
        return remote(owns[a].at[:, cols_1] if k == 0 else dst, dst, ys.at[a, way, k], yr.at[a, way, k], (s, beside))

    def cross_2(a):
        return remote(owns[a].at[:, cols_2], shard(a, row, z, cols_2), y2s.at[a], y2r.at[a], (s, beside))

    own_copies = [pltpu.make_async_copy(owns[a], shard(a, row, z, all_cols), own_sem.at[a]) for a in range(2)]
    for a in range(2):
        cross_2(a).start()
        for way in range(2):
            own_hop(a, way, 0).start()
        cross(a, 0, 0).start()
        own_copies[a].start()

    parity = lax.rem(z, 2)
    pairs = zn // 2

    def turn(a, line, step):
        shift = (0, 2 * parity - 1, 1 - 2 * parity, 2)[step]
        chunk = line * pairs + lax.rem(z // 2 + shift + pairs, pairs)
        span = pl.ds(pl.multiple_of(chunk * 2 * part, 2 * part), 2 * part)
        turned[a][:, span] = fulls[a][span, :].T

    def take_cross(a, k):
        for way in range(2):
            if (k > 0 or way == 0) and k <= reach[a][way]:
                wait_bytes(shard(a, 1 - row, ring_pos(way, k), cols_1), yr.at[a, way, k])

    for a in range(2):
        wait_bytes(shard(a, 1 - row, z, cols_2), y2r.at[a])
        for way in range(2):
            other_hop(a, way, 0).start()
    for a in range(2):
        own_copies[a].wait()

    for k in range(1, pairs + 1):
        for a in range(2):
            for way in range(2):
                if k <= reach[a][way]:
                    wait_bytes(shard(a, row, ring_pos(way, k), all_cols), zr.at[a, way, k - 1])
                    if k < reach[a][way]:
                        own_hop(a, way, k).start()
                    cross(a, way, k).start()
            for way in range(2):
                if k <= reach[a][way]:
                    wait_bytes(shard(a, 1 - row, ring_pos(way, k), cols_2), or_.at[a, way, k - 1])
                    if k < reach[a][way]:
                        other_hop(a, way, k).start()
        for a in range(2):
            take_cross(a, k - 1)
            turn(a, row, k - 1)
            if k > 1:
                turn(a, 1 - row, k - 2)
    for a in range(2):
        take_cross(a, pairs)
        turn(a, 1 - row, pairs - 1)

    gain_out[...] = jnp.zeros_like(gain_out)

    def incoming(i, b):
        return pl.ds(pl.multiple_of(b * rows_per, rows_per), rows_per)

    def await_from_above(i, b):
        @pl.when(not_last)
        def _():
            wait_bytes(rx.at[i, incoming(i, b)], p_recv.at[i, b])

    def give(i, b, rows, values):
        tx[i, rows] = values.astype(bf16)

        @pl.when(has_below)
        def _():
            remote(tx.at[i, rows], rx.at[i, rows], p_send.at[i], p_recv.at[i, b], (s - 1, d)).start()

    streams = jnp.logical_and(s < 4, jnp.logical_not(is_client))
    away = pl.ds(pl.multiple_of((1 - row) * hh, hh), hh)

    def norm_copy(q, a, rows):
        return remote(
            norm_full.at[q, a, rows, away], norm_cat.at[q, a, 1, rows],
            n_send.at[q, a], n_recv.at[q, a], (s, beside),
        )

    def delta_copy(q, a, rows):
        return remote(
            delta_cat.at[q, a, 0, rows], delta_cat.at[q, a, 1, rows],
            d_send.at[q, a], d_recv.at[q, a], (s, beside),
        )

    def norm_lend(a, b, rows):
        return remote(norm_full.at[0, a, rows], norm_full.at[1, a, rows], nl_send.at[a], nl_recv.at[a, b], (proxy, d))

    def delta_lend(a, b, rows):
        return remote(
            delta_cat.at[0, a, 0, rows], delta_cat.at[1, a, 0, rows], dl_send.at[a], dl_recv.at[a, b], (proxy, d)
        )

    def share_norm(a, b, rows, normed):
        norm_full[0, a, rows] = normed

        @pl.when(streams)
        def _():
            norm_copy(0, a, rows).start()

        @pl.when(is_client)
        def _():
            norm_lend(a, b, rows).start()

    def share_delta(a, b, rows):
        @pl.when(streams)
        def _():
            delta_copy(0, a, rows).start()

        @pl.when(is_client)
        def _():
            delta_lend(a, b, rows).start()

    first, second = pl.ds(0, h), pl.ds(h, h)

    def scale_of(values):
        return lax.rsqrt(jnp.sum(values * values, axis=-1, keepdims=True) * (1.0 / h) + offset)

    def pace(here):
        @pl.when(here)
        def _():
            pl.delay(1000)

    def upper_half(b, carry):
        rows = pl.ds(pl.multiple_of(b * rows_per, rows_per), rows_per)
        gain_f, gain_g = gains_ref[0:1, :], gains_ref[1:2, :]
        pace(jnp.logical_and(is_last, b > 0))
        await_from_above(1, b)
        await_from_above(0, b)
        y1 = jnp.where(is_last, pair_ref[rows, first], rx[0, rows].astype(f32))
        y2 = jnp.where(is_last, pair_ref[rows, second], rx[1, rows].astype(f32))
        y1s[rows] = y1
        r1 = scale_of(y1)
        pre_g = jnp.dot((y1 * gain_g).astype(bf16), wg[...], preferred_element_type=f32) * r1
        sig_g = jax.nn.sigmoid(pre_g)
        x2 = y2 - pre_g * sig_g
        give(1, b, rows, x2)
        r2 = scale_of(x2)
        pre_f = jnp.dot((x2 * gain_f).astype(bf16), wf[...], preferred_element_type=f32) * r2
        sig_f = jax.nn.sigmoid(pre_f)
        x1 = y1 - pre_f * sig_f
        give(0, b, rows, x1)
        in_pair_ref[rows, first] = x1
        in_pair_ref[rows, second] = x2
        pres[0, rows] = pre_g
        pres[1, rows] = pre_f
        slopes[0, rows] = sig_g * (1.0 + pre_g * (1.0 - sig_g))
        slopes[1, rows] = sig_f * (1.0 + pre_f * (1.0 - sig_f))
        share_norm(0, b, rows, (y1 * r1 * gain_g).astype(bf16))
        share_norm(1, b, rows, (x2 * r2 * gain_f).astype(bf16))

        return carry

    def lower_half(b, carry):
        rows = pl.ds(pl.multiple_of(b * rows_per, rows_per), rows_per)
        gain_f, gain_g = gains_ref[0:1, :], gains_ref[1:2, :]
        pace(jnp.logical_and(is_last, b > 0))
        await_from_above(2, b)
        await_from_above(3, b)
        gy1 = jnp.where(is_last, grad_ref[rows, first].astype(f32), rx[2, rows].astype(f32))
        gy2 = jnp.where(is_last, grad_ref[rows, second].astype(f32), rx[3, rows].astype(f32))
        delta_g = (gy2 * slopes[0, rows]).astype(bf16)
        back_g = jnp.dot(delta_g, wgt[...], preferred_element_type=f32)
        mean_g = jnp.sum(delta_g.astype(f32) * pres[0, rows], axis=-1, keepdims=True) * (1.0 / h)
        y1 = y1s[rows]
        r1 = scale_of(y1)
        gz = gy1 + (r1 * gain_g) * back_g - y1 * (mean_g * (r1 * r1))
        give(2, b, rows, gz)
        delta_f = (gz * slopes[1, rows]).astype(bf16)
        back_f = jnp.dot(delta_f, wft[...], preferred_element_type=f32)
        mean_f = jnp.sum(delta_f.astype(f32) * pres[1, rows], axis=-1, keepdims=True) * (1.0 / h)
        x2 = in_pair_ref[rows, second]
        r2 = scale_of(x2)
        gx2 = gy2 + (r2 * gain_f) * back_f - x2 * (mean_f * (r2 * r2))
        give(3, b, rows, gx2)
        in_grad_ref[rows, first] = gz.astype(bf16)
        in_grad_ref[rows, second] = gx2.astype(bf16)
        delta_cat[0, 0, 0, rows] = delta_g
        delta_cat[0, 1, 0, rows] = delta_f
        share_delta(0, b, rows)
        share_delta(1, b, rows)
        gain_out[1:2, :] += jnp.sum(back_g * (y1 * r1), axis=0, keepdims=True)
        gain_out[0:1, :] += jnp.sum(back_f * (x2 * r2), axis=0, keepdims=True)
        return carry

    lax.fori_loop(0, blocks, upper_half, 0)
    lax.fori_loop(0, blocks, lower_half, 0)

    @pl.when(has_below)
    def _():
        for i in range(4):
            wait_bytes(tx.at[i], p_send.at[i])

    upper = lax.rem(s, 2) == 1

    @pl.when(s >= 4)
    def _():
        @pl.when(jnp.logical_not(upper))
        def _():
            pl.semaphore_signal(turn_sem, inc=1, device_id=(s + 1, d), device_id_type=MESH)

        @pl.when(upper)
        def _():
            pl.semaphore_wait(turn_sem, 1)

        for a in range(2):
            norm_copy(0, a, pl.ds(0, tokens)).start()
            delta_copy(0, a, pl.ds(0, tokens)).start()

    gain_parts[d] = gain_out[...]
    for k in range(1, n):
        remote(gain_parts.at[d], gain_parts.at[d], c_send, c_recv, (s, lax.rem(d + k, n))).start()

    def slot(pos):
        return pl.ds(pl.multiple_of(pos * part, part), part)

    def sum_hop(q, a, way, t, c):
        return remote(
            rs_tx.at[q, a, way, t, c], rs_rx.at[q, a, way, t, c],
            r_send.at[q, a, way, t, c], r_recv.at[q, a, way, t, c], (s, ring_next[way]),
        )

    span = h // cuts

    def band(c):
        return pl.ds(c * span, span)

    def sum_pos(a, way, t):
        far = reach[a][way] - t
        return lax.rem(z + (far if way == 0 else zn - far), zn)

    def reduce_grads(q, emit):
        for a in range(2):
            wait_bytes(norm_cat.at[q, a, 1], n_recv.at[q, a])
            norm_cat[q, a, 0] = norm_full[q, a, :, pl.ds(pl.multiple_of(row * hh, hh), hh)]
            norm_turned[a] = norm_cat[q, a].reshape(2 * tokens, hh).T
        for a in range(2):
            wait_bytes(delta_cat.at[q, a, 1], d_recv.at[q, a])
            for c in range(cuts):
                sums[a, :, band(c)] = jnp.dot(
                    norm_turned[a], delta_cat[q, a, :, :, band(c)].reshape(2 * tokens, span), preferred_element_type=f32
                )
                for way in range(2):
                    if reach[a][way] > 0:
                        rs_tx[q, a, way, 0, c] = sums[a, slot(sum_pos(a, way, 0)), band(c)].astype(bf16)
                        sum_hop(q, a, way, 0, c).start()
        for t in range(1, pairs):
            for a in range(2):
                for c in range(cuts):
                    for way in range(2):
                        if t < reach[a][way]:
                            wait_bytes(rs_rx.at[q, a, way, t - 1, c], r_recv.at[q, a, way, t - 1, c])
                            rs_tx[q, a, way, t, c] = (
                                sums[a, slot(sum_pos(a, way, t)), band(c)] + rs_rx[q, a, way, t - 1, c].astype(f32)
                            ).astype(bf16)
                            sum_hop(q, a, way, t, c).start()
        for a in range(2):
            for c in range(cuts):
                total = sums[a, slot(z), band(c)]
                for way in range(2):
                    if reach[a][way] > 0:
                        last = reach[a][way] - 1
                        wait_bytes(rs_rx.at[q, a, way, last, c], r_recv.at[q, a, way, last, c])
                        total = total + rs_rx[q, a, way, last, c].astype(f32)
                emit(a, c, total)
        for a in range(2):
            wait_bytes(norm_cat.at[q, a, 1], n_send.at[q, a])
            wait_bytes(delta_cat.at[q, a, 1], d_send.at[q, a])
            for way in range(2):
                for k in range(reach[a][way]):
                    for c in range(cuts):
                        sum_hop(q, a, way, k, c).wait_send()

    grads = (g_out, f_out)

    def keep(a, c, total):
        grads[a][:, band(c)] = total

    def give_back(a, c):
        return remote(res_tx.at[a, c], res_rx.at[a, c], s_send.at[a, c], s_recv.at[a, c], (client, d))

    def lend_back(a, c, total):
        res_tx[a, c] = total.astype(bf16)
        give_back(a, c).start()

    @pl.when(jnp.logical_not(is_client))
    def _():
        reduce_grads(0, keep)

    @pl.when(is_proxy)
    def _():
        def lent_norms(b, carry):
            rows = pl.ds(pl.multiple_of(b * rows_per, rows_per), rows_per)
            for a in range(2):
                wait_bytes(norm_full.at[1, a, rows], nl_recv.at[a, b])
                norm_copy(1, a, rows).start()
            return carry

        def lent_deltas(b, carry):
            rows = pl.ds(pl.multiple_of(b * rows_per, rows_per), rows_per)
            for a in range(2):
                wait_bytes(delta_cat.at[1, a, 0, rows], dl_recv.at[a, b])
                delta_copy(1, a, rows).start()
            return carry

        lax.fori_loop(0, blocks, lent_norms, 0)
        lax.fori_loop(0, blocks, lent_deltas, 0)
        reduce_grads(1, lend_back)
        for a in range(2):
            for c in range(cuts):
                give_back(a, c).wait_send()

    @pl.when(is_client)
    def _():
        for a in range(2):
            for c in range(cuts):
                wait_bytes(res_rx.at[a, c], s_recv.at[a, c])
                grads[a][:, band(c)] = res_rx[a, c].astype(f32)
        for a in range(2):
            wait_bytes(norm_full.at[0, a], nl_send.at[a])
            wait_bytes(delta_cat.at[0, a, 0], dl_send.at[a])

    others = pl.ds(0, n - 1)
    wait_bytes(gain_parts.at[others], c_recv)
    total = gain_parts[0]
    for e in range(1, n):
        total = total + gain_parts[e]
    gain_out[...] = total

    wait_bytes(gain_parts.at[others], c_send)
    for a in range(2):
        cross_2(a).wait_send()
        cross(a, 0, 0).wait_send()
        for way in range(2):
            for k in range(reach[a][way]):
                own_hop(a, way, k).wait_send()
                other_hop(a, way, k).wait_send()
                cross(a, way, k + 1).wait_send()


def hand_over(*refs):
    n = (len(refs) - 2) // 3
    ins, outs, held, in_sem, out_sem = refs[:n], refs[n:2 * n], refs[2 * n:3 * n], refs[-2], refs[-1]
    loads = [pltpu.make_async_copy(ins[i], held[i], in_sem.at[i]) for i in range(n)]
    stores = [pltpu.make_async_copy(held[i], outs[i].at[0], out_sem.at[i]) for i in range(n)]
    for copy in loads:
        copy.start()
    for load, store in zip(loads, stores):
        load.wait()
        store.start()
    for copy in stores:
        copy.wait()


def shards(out_pair, out_grad, f_weight, g_weight, gains):
    n, sections = lax.axis_size("dp"), lax.axis_size("section")
    tokens, width = out_pair.shape
    h = width // 2
    part = f_weight.shape[1]
    blocks, cuts = 8, 2
    zn = n // 2
    hops = max(zn // 2, 1)
    vmem = pl.BlockSpec(memory_space=pltpu.VMEM)
    dma = pltpu.SemaphoreType.DMA
    outs = pl.pallas_call(
        functools.partial(kernel, n, sections, blocks, cuts),
        out_shape=(
            jax.ShapeDtypeStruct((tokens, width), f32),
            jax.ShapeDtypeStruct((tokens, width), bf16),
            jax.ShapeDtypeStruct((part, h), f32),
            jax.ShapeDtypeStruct((part, h), f32),
            jax.ShapeDtypeStruct((2, h), f32),
        ),
        in_specs=[vmem] * 5,
        out_specs=[vmem] * 5,
        scratch_shapes=[
            pltpu.VMEM((h, h), bf16),
            pltpu.VMEM((h, h), bf16),
            pltpu.VMEM((h, h), bf16),
            pltpu.VMEM((h, h), bf16),
            pltpu.VMEM((4, tokens, h), bf16),
            pltpu.VMEM((4, tokens, h), bf16),
            pltpu.VMEM((tokens, h), f32),
            pltpu.VMEM((2, tokens, h), f32),
            pltpu.VMEM((2, tokens, h), f32),
            pltpu.VMEM((2, 2, tokens, h), bf16),
            pltpu.VMEM((2, 2, 2, tokens, zn * part), bf16),
            pltpu.VMEM((2, 2, 2, tokens, h), bf16),
            pltpu.VMEM((2, zn * part, h), f32),
            pltpu.VMEM((2, zn * part, 2 * tokens), bf16),
            pltpu.VMEM((2, 2, 2, hops, cuts, part, h // cuts), bf16),
            pltpu.VMEM((2, 2, 2, hops, cuts, part, h // cuts), bf16),
            pltpu.VMEM((2, cuts, part, h // cuts), bf16),
            pltpu.VMEM((2, cuts, part, h // cuts), bf16),
            pltpu.VMEM((n, 2, h), f32),
            dma((2,)),
            dma((2, 2, hops)),
            dma((2, 2, hops)),
            dma((2, 2, hops)),
            dma((2, 2, hops)),
            dma((2, 2, hops + 1)),
            dma((2, 2, hops + 1)),
            dma((2,)),
            dma((2,)),
            dma((4,)),
            dma((4, blocks)),
            dma((2, 2)),
            dma((2, 2)),
            dma((2, 2)),
            dma((2, 2)),
            dma((2, 2, 2, hops, cuts)),
            dma((2, 2, 2, hops, cuts)),
            dma,
            dma,
            pltpu.SemaphoreType.REGULAR,
            dma((2,)),
            dma((2, blocks)),
            dma((2,)),
            dma((2, blocks)),
            dma((2, cuts)),
            dma((2, cuts)),
        ],
        compiler_params=pltpu.CompilerParams(
            collective_id=0, has_side_effects=True, vmem_limit_bytes=60 * 1024 * 1024
        ),
    )(out_pair, out_grad, f_weight[0], g_weight[0], gains[0])
    count = len(outs)
    return pl.pallas_call(
        hand_over,
        out_shape=tuple(jax.ShapeDtypeStruct((1,) + out.shape, out.dtype) for out in outs),
        in_specs=[pl.BlockSpec(memory_space=pl.ANY)] * count,
        out_specs=tuple([pl.BlockSpec(memory_space=pl.ANY)] * count),
        scratch_shapes=[pltpu.VMEM(out.shape, out.dtype) for out in outs] + [dma((count,)), dma((count,))],
    )(*outs)


def solution(mesh):
    placed = (
        P("dp", None),
        P("dp", None),
        P("section", "dp", None),
        P("section", "dp", None),
        P("section", None, None),
    )
    return jax.shard_map(
        shards,
        mesh=mesh,
        in_specs=placed,
        out_specs=(
            P("section", "dp", None),
            P("section", "dp", None),
            P("section", "dp", None),
            P("section", "dp", None),
            P("section", None, None),
        ),
        check_vma=False,
    )
```
